32 devices in a mesh: expert: 4 (over y, core), shard: 8 (over z, x).
Axes of the slice: x: 2, y: 2, z: 4, core: 2. Of those that a mesh axis runs over, the one named last changes fastest.
Arguments:
- master_gate: float32 [128, 2048, 768], P('expert', 'shard'), may hold values from -0.125 to 0.125
- second_gate: bfloat16 [128, 2048, 768], P('expert', 'shard'), may hold values from -0.0625 to 0.0625
- master_up: float32 [128, 2048, 768], P('expert', 'shard'), may hold values from -0.125 to 0.125
- second_up: bfloat16 [128, 2048, 768], P('expert', 'shard'), may hold values from -0.0625 to 0.0625
- router_weight: float32 [2048, 128], P('shard', 'expert'), may hold values from -0.125 to 0.125
- router_gain: float32 [2048], P('shard'), may hold values from 0.25 to 1.75
Outputs:
- final_gate: bfloat16 [128, 768, 2048], P('expert', 'shard')
- final_up: bfloat16 [128, 768, 2048], P('expert', 'shard')
- serve_router: bfloat16 [2048, 128], replicated
The draws below stay inside these ranges and needn't reach their ends.
All inputs are finite; a program needn't handle non-finite values.
Results may differ from the reference program's by a relative error of at most 0.001.
Values may be sent and summed in bfloat16 or wider, within the bound.
A program may use at most 192 MiB of HBM per device.

```python
import jax
import jax.numpy as jnp

EXPERTS = 128
D_MODEL = 2048
D_EXPERT = 768


def block_levels(own_key, shape, split, low, largest):
    factor_of = 1.0
    for position, parts in split:
        steps = jax.random.uniform(jax.random.fold_in(jax.random.fold_in(own_key, 6), position), (parts,), jnp.float32, low / len(split), largest / len(split))
        factor_of = factor_of * jnp.repeat(jnp.exp(steps), shape[position] // parts).reshape((-1,) + (1,) * (len(shape) - 1 - position))
    return factor_of


def scatter_about(stream_key, dims, width, bound, shards=(), dtype=jnp.bfloat16):
    entries = jax.random.normal(stream_key, dims, jnp.float32) * width
    if len(shards) > 0:
        entries = block_levels(stream_key, dims, shards, -0.22, 0.18) * entries
    return jnp.clip(entries, min=-bound, max=bound).astype(dtype)


def setup_inputs(seed: int = 0) -> dict:
    keys = jax.random.split(jax.random.key(seed), 7)
    master_gate = scatter_about(keys[0], (EXPERTS, D_MODEL, D_EXPERT), D_MODEL ** -0.5, 0.125, ((0, 4), (1, 8)), jnp.float32)
    second_gate = scatter_about(keys[1], (EXPERTS, D_MODEL, D_EXPERT), (D_MODEL * 4) ** -0.5, 0.0625, ((0, 4), (1, 8)))
    master_up = scatter_about(keys[2], (EXPERTS, D_MODEL, D_EXPERT), D_MODEL ** -0.5, 0.125, ((0, 4), (1, 8)), jnp.float32)
    second_up = scatter_about(keys[3], (EXPERTS, D_MODEL, D_EXPERT), (D_MODEL * 4) ** -0.5, 0.0625, ((0, 4), (1, 8)))
    router_weight = scatter_about(keys[4], (D_MODEL, EXPERTS), D_MODEL ** -0.5, 0.125, ((0, 8), (1, 4)), jnp.float32)
    router_gain = jnp.clip(1.0 + 0.15 * jax.random.normal(keys[5], (D_MODEL,), jnp.float32), 0.25, 1.75)
    return {"master_gate": master_gate, "second_gate": second_gate, "master_up": master_up, "second_up": second_up, "router_weight": router_weight, "router_gain": router_gain}


def reference(master_gate, second_gate, master_up, second_up, router_weight, router_gain):
    merged_gate = master_gate + second_gate.astype(jnp.float32)
    merged_up = master_up + second_up.astype(jnp.float32)
    final_gate = merged_gate.astype(jnp.bfloat16)
    final_gate = jnp.transpose(final_gate, (0, 2, 1))
    final_up = merged_up.astype(jnp.bfloat16)
    final_up = jnp.transpose(final_up, (0, 2, 1))
    serve_router = (router_weight * router_gain[:, None]).astype(jnp.bfloat16)
    return final_gate, final_up, serve_router
```

```python
import functools

import jax
import jax.numpy as jnp
from jax import lax
from jax.experimental import pallas as pl
from jax.experimental.pallas import tpu as pltpu
from jax.sharding import PartitionSpec as P

MESH = pl.DeviceIdType.MESH
SLOTS = 3
PIECES = 8
EXCHANGE_VMEM = 38 * 2**20
UNLOAD_VMEM = 4 * 2**20


def exchange_kernel(
    n, groups, mg, sg, mu, su, weight, gain, merged_all, own_block, router,
    wide, narrow, outbox, weight_in, gain_in, bands, turned_router,
    in_sem, send_sem, recv_sem, own_sem, rs_send, rs_recv, re_send, re_recv,
):
    experts, rows, _ = mg.shape
    block = outbox.shape[3]
    columns = weight.shape[0]
    me = lax.axis_index("shard")
    group = lax.axis_index("expert")

    def load(e):
        slot = lax.rem(e, SLOTS)
        return (
            pltpu.make_async_copy(mg.at[e], wide.at[slot, 0], in_sem.at[slot, 0]),
            pltpu.make_async_copy(sg.at[e], narrow.at[slot, 0], in_sem.at[slot, 1]),
            pltpu.make_async_copy(mu.at[e], wide.at[slot, 1], in_sem.at[slot, 2]),
            pltpu.make_async_copy(su.at[e], narrow.at[slot, 1], in_sem.at[slot, 3]),
        )

    barrier = pltpu.get_barrier_semaphore()
    for j in range(1, n):
        pl.semaphore_signal(barrier, inc=1, device_id=(group, lax.rem(me + j, n)), device_id_type=MESH)
    for j in range(1, groups):
        pl.semaphore_signal(barrier, inc=1, device_id=(lax.rem(group + j, groups), me), device_id_type=MESH)

    for e in range(SLOTS):
        for copy in load(e):
            copy.start()
    router_in = (
        pltpu.make_async_copy(weight, weight_in, own_sem.at[1]),
        pltpu.make_async_copy(gain, gain_in, own_sem.at[2]),
    )
    for copy in router_in:
        copy.start()
    for copy in router_in:
        copy.wait()
    band = bands.at[pl.ds(pl.multiple_of(group * columns, columns), columns)]
    cut = pl.ds(pl.multiple_of(me * rows, rows), rows)
    spot = band.at[:, cut]
    spot[...] = (weight_in[...] * gain_in[...]).astype(jnp.bfloat16)

    pl.semaphore_wait(barrier, n - 1 + groups - 1)

    half = n // 2
    lower = me < half
    near = [lax.rem(me + j, half) + jnp.where(lower, 0, half) for j in range(1, half)]
    far = [lax.rem(me + j, half) + jnp.where(lower, half, 0) for j in range(half)]

    def send(e):
        for peer in far + near:
            pltpu.make_async_remote_copy(
                src_ref=outbox.at[peer, e], dst_ref=merged_all.at[e, :, :, cut],
                send_sem=send_sem.at[peer], recv_sem=recv_sem.at[me],
                device_id=(group, peer), device_id_type=MESH,
            ).start()

    def step(e, _):
        slot = lax.rem(e, SLOTS)
        for copy in load(e):
            copy.wait()
        for which in range(2):
            merged = wide[slot, which] + narrow[slot, which].astype(jnp.float32)
            turned = merged.astype(jnp.bfloat16).T
            for d in range(n):
                outbox[d, e, which] = turned[d * block:(d + 1) * block]

        @pl.when(e + SLOTS < experts)
        def _():
            for copy in load(e + SLOTS):
                copy.start()

        @pl.when(e > 0)
        def _():
            send(e - 1)

        return 0

    step(0, 0)
    router_rows = []
    for j in range(1, n):
        router_rows.append(
            pltpu.make_async_remote_copy(
                src_ref=spot, dst_ref=spot, send_sem=rs_send.at[j], recv_sem=rs_recv.at[j],
                device_id=(group, lax.rem(me + j, n)), device_id_type=MESH,
            )
        )
        router_rows[-1].start()
    lax.fori_loop(1, experts, step, 0)
    send(experts - 1)

    own = pltpu.make_async_copy(outbox.at[me], own_block, own_sem.at[0])
    own.start()

    for copy in router_rows:
        copy.wait()
    router_bands = []
    for j in range(1, groups):
        router_bands.append(
            pltpu.make_async_remote_copy(
                src_ref=band, dst_ref=band, send_sem=re_send.at[j], recv_sem=re_recv.at[j],
                device_id=(lax.rem(group + j, groups), me), device_id_type=MESH,
            )
        )
        router_bands[-1].start()
    own.wait()
    own = pltpu.make_async_copy(own_block, merged_all.at[:, :, :, cut], own_sem.at[0])
    own.start()
    for copy in router_bands:
        copy.wait()
    for d in range(n):
        turned_router[d * rows:(d + 1) * rows] = bands[:, d * rows:(d + 1) * rows].T
    out_router = pltpu.make_async_copy(turned_router, router, own_sem.at[1])
    out_router.start()

    own.wait()
    out_router.wait()
    for j in range(1, n):
        peer = lax.rem(me + j, n)
        pltpu.make_async_copy(outbox.at[peer], outbox.at[peer], send_sem.at[peer]).wait()
        landed = merged_all.at[:, :, :, pl.ds(pl.multiple_of(peer * rows, rows), rows)]
        pltpu.make_async_copy(landed, landed, recv_sem.at[peer]).wait()


def unload_kernel(merged_all, router_in, gate, up, router, buffer, sem, router_sem):
    experts = merged_all.shape[0]
    pieces = sem.shape[1]
    some = experts // pieces
    fetch = pltpu.make_async_copy(router_in, buffer, router_sem.at[0])
    fetch.start()
    copies = []
    for i in range(pieces):
        part = pl.ds(i * some, some)
        for which, out in enumerate((gate, up)):
            copies.append(pltpu.make_async_copy(merged_all.at[part, which], out.at[part], sem.at[which, i]))
            copies[-1].start()
    fetch.wait()
    store = pltpu.make_async_copy(buffer, router, router_sem.at[1])
    store.start()
    for copy in copies:
        copy.wait()
    store.wait()


def by_kernel(n, groups, master_gate, second_gate, master_up, second_up, router_weight, router_gain):
    experts, rows, width = master_gate.shape
    block = width // n
    columns = router_weight.shape[1]
    anywhere = pl.BlockSpec(memory_space=pl.ANY)
    dma = pltpu.SemaphoreType.DMA
    bf16 = jnp.bfloat16
    merged_all, _, router = pl.pallas_call(
        functools.partial(exchange_kernel, n, groups),
        out_shape=(
            pltpu.VMEM((experts, 2, block, n * rows), bf16),
            pltpu.HBM((experts, 2, block, rows), bf16),
            pltpu.HBM((n * rows, groups * columns), bf16),
        ),
        in_specs=[anywhere] * 6,
        out_specs=(anywhere,) * 3,
        scratch_shapes=[
            pltpu.VMEM((SLOTS, 2, rows, width), jnp.float32),
            pltpu.VMEM((SLOTS, 2, rows, width), bf16),
            pltpu.VMEM((n, experts, 2, block, rows), bf16),
            pltpu.VMEM((columns, rows), jnp.float32),
            pltpu.VMEM((1, rows), jnp.float32),
            pltpu.VMEM((groups * columns, n * rows), bf16),
            pltpu.VMEM((n * rows, groups * columns), bf16),
            dma((SLOTS, 4)), dma((n,)), dma((n,)), dma((3,)),
            dma((n,)), dma((n,)), dma((groups,)), dma((groups,)),
        ],
        compiler_params=pltpu.CompilerParams(
            collective_id=0, has_side_effects=True, vmem_limit_bytes=EXCHANGE_VMEM
        ),
    )(master_gate, second_gate, master_up, second_up, router_weight.T, router_gain[None])
    pieces = PIECES if experts % PIECES == 0 else 1
    whole = jax.ShapeDtypeStruct((experts, block, n * rows), bf16)
    return pl.pallas_call(
        unload_kernel,
        out_shape=(whole, whole, jax.ShapeDtypeStruct(router.shape, bf16)),
        in_specs=[anywhere] * 2,
        out_specs=(anywhere,) * 3,
        scratch_shapes=[pltpu.VMEM(router.shape, bf16), dma((2, pieces)), dma((2,))],
        compiler_params=pltpu.CompilerParams(vmem_limit_bytes=UNLOAD_VMEM),
    )(pltpu.with_memory_space_constraint(merged_all, pltpu.VMEM), pltpu.with_memory_space_constraint(router, pltpu.HBM))


def by_collectives(master_gate, second_gate, master_up, second_up, part):
    def moved(master, second):
        narrow = (master + second.astype(jnp.float32)).astype(jnp.bfloat16)
        sent = lax.all_to_all(narrow, "shard", split_axis=2, concat_axis=1, tiled=True)
        return jnp.transpose(sent, (0, 2, 1))

    bands = lax.all_gather(part.T, "shard", axis=0, tiled=True)
    router = lax.all_gather(bands, "expert", axis=1, tiled=True)
    return moved(master_gate, second_gate), moved(master_up, second_up), router


def per_device(n, groups, master_gate, second_gate, master_up, second_up, router_weight, router_gain):
    experts, rows, width = master_gate.shape
    columns = router_weight.shape[1]
    fits = n >= 4 and n % 4 == 0 and groups > 1 and rows % 128 == 0 and width % (16 * n) == 0
    fits = fits and columns % 16 == 0 and experts > SLOTS
    fits = fits and experts * rows * width * 4 <= 24 * 2**20 and SLOTS * rows * width * 12 <= 7 * 2**20
    fits = fits and n * rows * groups * columns * 2 <= 2**20
    if fits:
        return by_kernel(n, groups, master_gate, second_gate, master_up, second_up, router_weight, router_gain)
    part = (router_weight * router_gain[:, None]).astype(jnp.bfloat16).T
    return by_collectives(master_gate, second_gate, master_up, second_up, part)


def solution(mesh):
    placed = (
        P("expert", "shard", None),
        P("expert", "shard", None),
        P("expert", "shard", None),
        P("expert", "shard", None),
        P("shard", "expert"),
        P("shard"),
    )
    return jax.shard_map(
        functools.partial(per_device, mesh.shape["shard"], mesh.shape["expert"]),
        mesh=mesh,
        in_specs=placed,
        out_specs=(P("expert", "shard", None), P("expert", "shard", None), P()),
        check_vma=False,
    )
```

```python
import functools

import jax
import jax.numpy as jnp
from jax import lax
from jax.experimental import pallas as pl
from jax.experimental.pallas import tpu as pltpu
from jax.sharding import PartitionSpec as P

MESH = pl.DeviceIdType.MESH
SLOTS = 3
LATE = (8, 4)
EXCHANGE_VMEM = 38 * 2**20
UNLOAD_VMEM = 4 * 2**20


def late_experts(group):
    return jnp.where(lax.rem(group, 2) == 0, LATE[0], LATE[1])


def exchange_kernel(n, groups, first, *refs):
    mg, sg, mu, su, *refs = refs
    if first:
        weight, gain, landed, own_block, router, *refs = refs
        wide, narrow, outbox, *refs = refs
        weight_in, gain_in, bands, turned_router, *refs = refs
        in_sem, send_sem, recv_sem, own_out, own_back, router_sem, rs_send, rs_recv, re_send, re_recv = refs
    else:
        _, landed, own_block, *refs = refs
        wide, narrow, outbox, in_sem, send_sem, recv_sem, own_out, own_back = refs
    experts, rows, _ = mg.shape
    block = outbox.shape[3]
    me = lax.axis_index("shard")
    group = lax.axis_index("expert")
    late = late_experts(group)
    base = 0 if first else experts - late
    count = experts - late if first else late

    barrier = pltpu.get_barrier_semaphore()
    for j in range(1, n):
        pl.semaphore_signal(barrier, inc=1, device_id=(group, lax.rem(me + j, n)), device_id_type=MESH)
    if first:
        for j in range(1, groups):
            pl.semaphore_signal(barrier, inc=1, device_id=(lax.rem(group + j, groups), me), device_id_type=MESH)

    def load(e):
        slot = lax.rem(e, SLOTS)
        return (
            pltpu.make_async_copy(mg.at[base + e], wide.at[slot, 0], in_sem.at[slot, 0]),
            pltpu.make_async_copy(sg.at[base + e], narrow.at[slot, 0], in_sem.at[slot, 1]),
            pltpu.make_async_copy(mu.at[base + e], wide.at[slot, 1], in_sem.at[slot, 2]),
            pltpu.make_async_copy(su.at[base + e], narrow.at[slot, 1], in_sem.at[slot, 3]),
        )

    for e in range(SLOTS):
        for copy in load(e):
            copy.start()
    cut = pl.ds(pl.multiple_of(me * rows, rows), rows)
    if first:
        router_in = (
            pltpu.make_async_copy(weight, weight_in, router_sem.at[0]),
            pltpu.make_async_copy(gain, gain_in, router_sem.at[1]),
        )
        for copy in router_in:
            copy.start()
        columns = weight.shape[0]
        band = bands.at[pl.ds(pl.multiple_of(group * columns, columns), columns)]
        spot = band.at[:, cut]

    half = n // 2
    lower = me < half
    near = [lax.rem(me + j, half) + jnp.where(lower, 0, half) for j in range(1, half)]
    far = [j + jnp.where(lower, half, 0) for j in range(half)]

    def remote(src, dst, e, peer):
        return pltpu.make_async_remote_copy(
            src_ref=src, dst_ref=dst, send_sem=send_sem.at[e], recv_sem=recv_sem.at[e],
            device_id=(group, peer), device_id_type=MESH,
        )

    def send(e):
        for peer in far + near:
            remote(outbox.at[peer, e], landed.at[e, :, :, cut], e, peer).start()

    def send_half(e, which):
        for peer in far + near:
            remote(outbox.at[peer, e, which], landed.at[e, which, :, cut], e, peer).start()

    def turn(e, which):
        slot = lax.rem(e, SLOTS)
        merged = wide[slot, which] + narrow[slot, which].astype(jnp.float32)
        turned = merged.astype(jnp.bfloat16).T
        for d in range(n):
            outbox[d, e, which] = turned[d * block:(d + 1) * block]

    def step(e, _):
        for copy in load(e):
            copy.wait()
        for which in range(2):
            turn(e, which)

        @pl.when(e + SLOTS < count)
        def _():
            for copy in load(e + SLOTS):
                copy.start()

        @pl.when(e > 1)
        def _():
            send(e - 1)

        return 0

    opening = load(0)
    for which in range(2):
        for copy in opening[2 * which:2 * which + 2]:
            copy.wait()
        turn(0, which)

    @pl.when(SLOTS < count)
    def _():
        for copy in load(SLOTS):
            copy.start()

    pl.semaphore_wait(barrier, n - 1 + (groups - 1 if first else 0))
    send_half(0, 0)
    if first:
        for copy in router_in:
            copy.wait()
        spot[...] = (weight_in[...] * gain_in[...]).astype(jnp.bfloat16)
    step(1, 0)
    send_half(0, 1)
    if first:
        router_rows = []
        for j in range(1, n):
            router_rows.append(
                pltpu.make_async_remote_copy(
                    src_ref=spot, dst_ref=spot, send_sem=rs_send.at[j], recv_sem=rs_recv.at[j],
                    device_id=(group, lax.rem(me + j, n)), device_id_type=MESH,
                )
            )
            router_rows[-1].start()
    lax.fori_loop(2, count, step, 0)
    send(count - 1)

    def leave(e):
        return pltpu.make_async_copy(outbox.at[me, e], own_block.at[e], own_out.at[e])

    def back(e):
        return pltpu.make_async_copy(own_block.at[e], landed.at[e, :, :, cut], own_back.at[e])

    def own_leave(e, _):
        leave(e).start()
        return 0

    def own_return(e, _):
        leave(e).wait()
        back(e).start()
        return 0

    lax.fori_loop(0, count, own_leave, 0)
    lax.fori_loop(0, count, own_return, 0)

    if first:
        for copy in router_rows:
            copy.wait()
        router_bands = []
        for j in range(1, groups):
            router_bands.append(
                pltpu.make_async_remote_copy(
                    src_ref=band, dst_ref=band, send_sem=re_send.at[j], recv_sem=re_recv.at[j],
                    device_id=(lax.rem(group + j, groups), me), device_id_type=MESH,
                )
            )
            router_bands[-1].start()
        for copy in router_bands:
            copy.wait()
        for d in range(n):
            turned_router[d * rows:(d + 1) * rows] = bands[:, d * rows:(d + 1) * rows].T
        out_router = pltpu.make_async_copy(turned_router, router, router_sem.at[0])
        out_router.start()
        out_router.wait()

    def finish(e, _):
        back(e).wait()
        gone = outbox.at[pl.ds(0, n - 1), e]
        pltpu.make_async_copy(gone, gone, send_sem.at[e]).wait()
        come = landed.at[e, :, :, pl.ds(0, (n - 1) * rows)]
        pltpu.make_async_copy(come, come, recv_sem.at[e]).wait()
        return 0

    lax.fori_loop(0, count, finish, 0)


def unload_kernel(first, *refs):
    if first:
        landed, router_in, gate, up, router, token, buffer, sem, router_sem = refs
    else:
        landed, _, _, gate, up, sem = refs
    experts = gate.shape[0]
    late = late_experts(lax.axis_index("expert"))
    base = 0 if first else experts - late
    count = experts - late if first else late

    def copies(e):
        return (
            pltpu.make_async_copy(landed.at[e, 0], gate.at[base + e], sem.at[0, e]),
            pltpu.make_async_copy(landed.at[e, 1], up.at[base + e], sem.at[1, e]),
        )

    def start(e, _):
        for copy in copies(e):
            copy.start()
        return 0

    def wait(e, _):
        for copy in copies(e):
            copy.wait()
        return 0

    if first:
        fetch = pltpu.make_async_copy(router_in, buffer, router_sem.at[0])
        fetch.start()
    lax.fori_loop(0, count, start, 0)
    if first:
        token[...] = jnp.zeros_like(token)
        fetch.wait()
        store = pltpu.make_async_copy(buffer, router, router_sem.at[1])
        store.start()
        store.wait()
    lax.fori_loop(0, count, wait, 0)


def by_kernel(n, groups, master_gate, second_gate, master_up, second_up, router_weight, router_gain):
    experts, rows, width = master_gate.shape
    block = width // n
    columns = router_weight.shape[1]
    anywhere = pl.BlockSpec(memory_space=pl.ANY)
    dma = pltpu.SemaphoreType.DMA
    bf16 = jnp.bfloat16
    whole = jax.ShapeDtypeStruct((experts, block, n * rows), bf16)
    router_shape = (n * rows, groups * columns)
    token_shape = jax.ShapeDtypeStruct((8, 128), jnp.float32)
    stay = functools.partial(pltpu.with_memory_space_constraint, memory_space=pltpu.HBM)
    masters = tuple(stay(x) for x in (master_gate, second_gate, master_up, second_up))

    def exchange(first, most, more, extra_out, extra_scratch, extra_sems):
        return pl.pallas_call(
            functools.partial(exchange_kernel, n, groups, first),
            out_shape=(
                pltpu.VMEM((most, 2, block, n * rows), bf16),
                pltpu.HBM((most, 2, block, rows), bf16),
                *extra_out,
            ),
            in_specs=[anywhere] * (4 + len(more)),
            out_specs=(anywhere,) * (2 + len(extra_out)),
            scratch_shapes=[
                pltpu.VMEM((SLOTS, 2, rows, width), jnp.float32),
                pltpu.VMEM((SLOTS, 2, rows, width), bf16),
                pltpu.VMEM((n, most, 2, block, rows), bf16),
                *extra_scratch,
                dma((SLOTS, 4)), dma((most,)), dma((most,)), dma((most,)), dma((most,)),
                *extra_sems,
            ],
            compiler_params=pltpu.CompilerParams(
                collective_id=0 if first else 1, has_side_effects=True, vmem_limit_bytes=EXCHANGE_VMEM
            ),
        )(*masters, *more)

    most = experts - min(LATE)
    landed, _, router = exchange(
        True, most, (stay(router_weight.T), stay(router_gain[None])),
        (pltpu.HBM(router_shape, bf16),),
        (
            pltpu.VMEM((columns, rows), jnp.float32),
            pltpu.VMEM((1, rows), jnp.float32),
            pltpu.VMEM((groups * columns, n * rows), bf16),
            pltpu.VMEM(router_shape, bf16),
        ),
        (dma((2,)), dma((n,)), dma((n,)), dma((groups,)), dma((groups,))),
    )
    gate, up, router, token = pl.pallas_call(
        functools.partial(unload_kernel, True),
        out_shape=(whole, whole, jax.ShapeDtypeStruct(router_shape, bf16), token_shape),
        in_specs=[anywhere] * 2,
        out_specs=(anywhere,) * 3 + (pl.BlockSpec(memory_space=pltpu.VMEM),),
        scratch_shapes=[pltpu.VMEM(router_shape, bf16), dma((2, most)), dma((2,))],
        compiler_params=pltpu.CompilerParams(vmem_limit_bytes=UNLOAD_VMEM),
    )(pltpu.with_memory_space_constraint(landed, pltpu.VMEM), stay(router))
    landed, _ = exchange(False, max(LATE), (token,), (), (), ())
    gate, up = pl.pallas_call(
        functools.partial(unload_kernel, False),
        out_shape=(whole, whole),
        in_specs=[anywhere] * 3,
        out_specs=(anywhere,) * 2,
        scratch_shapes=[dma((2, max(LATE)))],
        input_output_aliases={1: 0, 2: 1},
        compiler_params=pltpu.CompilerParams(vmem_limit_bytes=UNLOAD_VMEM),
    )(pltpu.with_memory_space_constraint(landed, pltpu.VMEM), stay(gate), stay(up))
    return gate, up, router


def by_collectives(master_gate, second_gate, master_up, second_up, part):
    def moved(master, second):
        narrow = (master + second.astype(jnp.float32)).astype(jnp.bfloat16)
        sent = lax.all_to_all(narrow, "shard", split_axis=2, concat_axis=1, tiled=True)
        return jnp.transpose(sent, (0, 2, 1))

    bands = lax.all_gather(part.T, "shard", axis=0, tiled=True)
    router = lax.all_gather(bands, "expert", axis=1, tiled=True)
    return moved(master_gate, second_gate), moved(master_up, second_up), router


def per_device(n, groups, master_gate, second_gate, master_up, second_up, router_weight, router_gain):
    experts, rows, width = master_gate.shape
    columns = router_weight.shape[1]
    fits = n >= 4 and n % 4 == 0 and groups > 1 and rows % 128 == 0 and width % (16 * n) == 0
    fits = fits and columns % 16 == 0 and min(LATE) >= SLOTS and experts - max(LATE) > SLOTS
    fits = fits and experts * rows * width * 4 <= 24 * 2**20 and SLOTS * rows * width * 12 <= 7 * 2**20
    fits = fits and n * rows * groups * columns * 2 <= 2**20
    if fits:
        return by_kernel(n, groups, master_gate, second_gate, master_up, second_up, router_weight, router_gain)
    part = (router_weight * router_gain[:, None]).astype(jnp.bfloat16).T
    return by_collectives(master_gate, second_gate, master_up, second_up, part)


def solution(mesh):
    placed = (
        P("expert", "shard", None),
        P("expert", "shard", None),
        P("expert", "shard", None),
        P("expert", "shard", None),
        P("shard", "expert"),
        P("shard"),
    )
    return jax.shard_map(
        functools.partial(per_device, mesh.shape["shard"], mesh.shape["expert"]),
        mesh=mesh,
        in_specs=placed,
        out_specs=(P("expert", "shard", None), P("expert", "shard", None), P()),
        check_vma=False,
    )
```

```python
import functools

import jax
import jax.numpy as jnp
from jax import lax
from jax.experimental import pallas as pl
from jax.experimental.pallas import tpu as pltpu
from jax.sharding import PartitionSpec as P

MESH = pl.DeviceIdType.MESH
SLOTS = 3
LATE = (6, 2)
EXCHANGE_VMEM = 38 * 2**20
UNLOAD_VMEM = 4 * 2**20


def late_experts(group):
    return jnp.where(lax.rem(group, 2) == 0, LATE[0], LATE[1])


def exchange_kernel(n, groups, first, *refs):
    mg, sg, mu, su, *refs = refs
    if first:
        weight, gain, landed, own_block, router, *refs = refs
        wide, narrow, outbox, *refs = refs
        weight_in, gain_in, bands, turned_router, *refs = refs
        in_sem, send_sem, recv_sem, own_out, own_back, router_sem, rs_send, rs_recv, rl_send, rl_recv, re_send, re_recv = refs
    else:
        _, landed, own_block, *refs = refs
        wide, narrow, outbox, in_sem, send_sem, recv_sem, own_out, own_back = refs
    experts, rows, _ = mg.shape
    slots = wide.shape[0]
    block = outbox.shape[3]
    me = lax.axis_index("shard")
    group = lax.axis_index("expert")
    late = late_experts(group)
    base = 0 if first else experts - late
    count = experts - late if first else late

    barrier = pltpu.get_barrier_semaphore()
    for j in range(1, n):
        pl.semaphore_signal(barrier, inc=1, device_id=(group, lax.rem(me + j, n)), device_id_type=MESH)
    if first:
        for j in range(1, groups):
            pl.semaphore_signal(barrier, inc=1, device_id=(lax.rem(group + j, groups), me), device_id_type=MESH)

    def load(e):
        slot = lax.rem(e, slots)
        return (
            pltpu.make_async_copy(mg.at[base + e], wide.at[slot, 0], in_sem.at[slot, 0]),
            pltpu.make_async_copy(sg.at[base + e], narrow.at[slot, 0], in_sem.at[slot, 1]),
            pltpu.make_async_copy(mu.at[base + e], wide.at[slot, 1], in_sem.at[slot, 2]),
            pltpu.make_async_copy(su.at[base + e], narrow.at[slot, 1], in_sem.at[slot, 3]),
        )

    for e in range(slots):
        for copy in load(e):
            copy.start()
    cut = pl.ds(pl.multiple_of(me * rows, rows), rows)
    if first:
        router_in = (
            pltpu.make_async_copy(weight, weight_in, router_sem.at[0]),
            pltpu.make_async_copy(gain, gain_in, router_sem.at[1]),
        )
        for copy in router_in:
            copy.start()
        columns = weight.shape[0]
        band = bands.at[pl.ds(pl.multiple_of(group * columns, columns), columns)]
        spot = band.at[:, cut]

    half = n // 2
    lower = me < half
    near = [lax.rem(me + j, half) + jnp.where(lower, 0, half) for j in range(1, half)]
    far = [j + jnp.where(lower, half, 0) for j in range(half)]

    def remote(src, dst, e, peer):
        return pltpu.make_async_remote_copy(
            src_ref=src, dst_ref=dst, send_sem=send_sem.at[e], recv_sem=recv_sem.at[e],
            device_id=(group, peer), device_id_type=MESH,
        )

    def send(e):
        for peer in far + near:
            remote(outbox.at[peer, e], landed.at[e, :, :, cut], e, peer).start()

    def send_half(e, which):
        for peer in far + near:
            remote(outbox.at[peer, e, which], landed.at[e, which, :, cut], e, peer).start()

    def turn(e, which):
        slot = lax.rem(e, slots)
        merged = wide[slot, which] + narrow[slot, which].astype(jnp.float32)
        turned = merged.astype(jnp.bfloat16).T
        for d in range(n):
            outbox[d, e, which] = turned[d * block:(d + 1) * block]

    def step(e, _):
        for copy in load(e):
            copy.wait()
        for which in range(2):
            turn(e, which)

        @pl.when(e + slots < count)
        def _():
            for copy in load(e + slots):
                copy.start()

        @pl.when(e > 1)
        def _():
            send(e - 1)

        return 0

    opening = load(0)
    for which in range(2):
        for copy in opening[2 * which:2 * which + 2]:
            copy.wait()
        turn(0, which)

    @pl.when(slots < count)
    def _():
        for copy in load(slots):
            copy.start()

    pl.semaphore_wait(barrier, n - 1 + (groups - 1 if first else 0))
    send_half(0, 0)
    if first:
        for copy in router_in:
            copy.wait()
        spot[...] = (weight_in[...] * gain_in[...]).astype(jnp.bfloat16)
    step(1, 0)
    send_half(0, 1)
    if first:
        partner = lax.rem(me + half, n)
        router_rows = []
        for j, peer in enumerate([partner] + near):
            router_rows.append(
                pltpu.make_async_remote_copy(
                    src_ref=spot, dst_ref=spot, send_sem=rs_send.at[j], recv_sem=rs_recv.at[j],
                    device_id=(group, peer), device_id_type=MESH,
                )
            )
            router_rows[-1].start()
        lax.fori_loop(2, SLOTS + 1, step, 0)
        router_rows[0].wait()
        passed = band.at[:, pl.ds(pl.multiple_of(partner * rows, rows), rows)]
        for j, peer in enumerate(near):
            router_rows.append(
                pltpu.make_async_remote_copy(
                    src_ref=passed, dst_ref=passed, send_sem=rl_send.at[j], recv_sem=rl_recv.at[j],
                    device_id=(group, peer), device_id_type=MESH,
                )
            )
            router_rows[-1].start()
    lax.fori_loop(SLOTS + 1 if first else 2, count, step, 0)
    send(count - 1)

    def leave(e):
        return pltpu.make_async_copy(outbox.at[me, e], own_block.at[e], own_out.at[e])

    def back(e):
        return pltpu.make_async_copy(own_block.at[e], landed.at[e, :, :, cut], own_back.at[e])

    def own_leave(e, _):
        leave(e).start()
        return 0

    def own_return(e, _):
        leave(e).wait()
        back(e).start()
        return 0

    lax.fori_loop(0, count, own_leave, 0)
    lax.fori_loop(0, count, own_return, 0)

    if first:
        for copy in router_rows[1:]:
            copy.wait()
        router_bands = []
        for j in range(1, groups):
            router_bands.append(
                pltpu.make_async_remote_copy(
                    src_ref=band, dst_ref=band, send_sem=re_send.at[j], recv_sem=re_recv.at[j],
                    device_id=(lax.rem(group + j, groups), me), device_id_type=MESH,
                )
            )
            router_bands[-1].start()
        for copy in router_bands:
            copy.wait()
        for d in range(n):
            turned_router[d * rows:(d + 1) * rows] = bands[:, d * rows:(d + 1) * rows].T
        out_router = pltpu.make_async_copy(turned_router, router, router_sem.at[0])
        out_router.start()
        out_router.wait()

    def finish(e, _):
        back(e).wait()
        gone = outbox.at[pl.ds(0, n - 1), e]
        pltpu.make_async_copy(gone, gone, send_sem.at[e]).wait()
        come = landed.at[e, :, :, pl.ds(0, (n - 1) * rows)]
        pltpu.make_async_copy(come, come, recv_sem.at[e]).wait()
        return 0

    lax.fori_loop(0, count, finish, 0)


def unload_kernel(first, *refs):
    if first:
        landed, router_in, gate, up, router, token, buffer, sem, router_sem = refs
    else:
        landed, _, _, gate, up, sem = refs
    experts = gate.shape[0]
    late = late_experts(lax.axis_index("expert"))
    base = 0 if first else experts - late
    count = experts - late if first else late

    def copies(e):
        return (
            pltpu.make_async_copy(landed.at[e, 0], gate.at[base + e], sem.at[0, e]),
            pltpu.make_async_copy(landed.at[e, 1], up.at[base + e], sem.at[1, e]),
        )

    def start(e, _):
        for copy in copies(e):
            copy.start()
        return 0

    def wait(e, _):
        for copy in copies(e):
            copy.wait()
        return 0

    if first:
        fetch = pltpu.make_async_copy(router_in, buffer, router_sem.at[0])
        fetch.start()
    lax.fori_loop(0, count, start, 0)
    if first:
        token[...] = jnp.zeros_like(token)
        fetch.wait()
        store = pltpu.make_async_copy(buffer, router, router_sem.at[1])
        store.start()
        store.wait()
    lax.fori_loop(0, count, wait, 0)


def by_kernel(n, groups, master_gate, second_gate, master_up, second_up, router_weight, router_gain):
    experts, rows, width = master_gate.shape
    block = width // n
    columns = router_weight.shape[1]
    anywhere = pl.BlockSpec(memory_space=pl.ANY)
    dma = pltpu.SemaphoreType.DMA
    bf16 = jnp.bfloat16
    whole = jax.ShapeDtypeStruct((experts, block, n * rows), bf16)
    router_shape = (n * rows, groups * columns)
    token_shape = jax.ShapeDtypeStruct((8, 128), jnp.float32)
    stay = functools.partial(pltpu.with_memory_space_constraint, memory_space=pltpu.HBM)
    masters = tuple(stay(x) for x in (master_gate, second_gate, master_up, second_up))

    def exchange(first, most, more, extra_out, extra_scratch, extra_sems):
        slots = SLOTS if first else min(SLOTS, *LATE)
        return pl.pallas_call(
            functools.partial(exchange_kernel, n, groups, first),
            out_shape=(
                pltpu.VMEM((most, 2, block, n * rows), bf16),
                pltpu.HBM((most, 2, block, rows), bf16),
                *extra_out,
            ),
            in_specs=[anywhere] * (4 + len(more)),
            out_specs=(anywhere,) * (2 + len(extra_out)),
            scratch_shapes=[
                pltpu.VMEM((slots, 2, rows, width), jnp.float32),
                pltpu.VMEM((slots, 2, rows, width), bf16),
                pltpu.VMEM((n, most, 2, block, rows), bf16),
                *extra_scratch,
                dma((slots, 4)), dma((most,)), dma((most,)), dma((most,)), dma((most,)),
                *extra_sems,
            ],
            compiler_params=pltpu.CompilerParams(
                collective_id=0 if first else 1, has_side_effects=True, vmem_limit_bytes=EXCHANGE_VMEM
            ),
        )(*masters, *more)

    most = experts - min(LATE)
    landed, _, router = exchange(
        True, most, (stay(router_weight.T), stay(router_gain[None])),
        (pltpu.HBM(router_shape, bf16),),
        (
            pltpu.VMEM((columns, rows), jnp.float32),
            pltpu.VMEM((1, rows), jnp.float32),
            pltpu.VMEM((groups * columns, n * rows), bf16),
            pltpu.VMEM(router_shape, bf16),
        ),
        (dma((2,)), *[dma((n // 2,))] * 4, dma((groups,)), dma((groups,))),
    )
    gate, up, router, token = pl.pallas_call(
        functools.partial(unload_kernel, True),
        out_shape=(whole, whole, jax.ShapeDtypeStruct(router_shape, bf16), token_shape),
        in_specs=[anywhere] * 2,
        out_specs=(anywhere,) * 3 + (pl.BlockSpec(memory_space=pltpu.VMEM),),
        scratch_shapes=[pltpu.VMEM(router_shape, bf16), dma((2, most)), dma((2,))],
        compiler_params=pltpu.CompilerParams(vmem_limit_bytes=UNLOAD_VMEM),
    )(pltpu.with_memory_space_constraint(landed, pltpu.VMEM), stay(router))
    landed, _ = exchange(False, max(LATE), (token,), (), (), ())
    gate, up = pl.pallas_call(
        functools.partial(unload_kernel, False),
        out_shape=(whole, whole),
        in_specs=[anywhere] * 3,
        out_specs=(anywhere,) * 2,
        scratch_shapes=[dma((2, max(LATE)))],
        input_output_aliases={1: 0, 2: 1},
        compiler_params=pltpu.CompilerParams(vmem_limit_bytes=UNLOAD_VMEM),
    )(pltpu.with_memory_space_constraint(landed, pltpu.VMEM), stay(gate), stay(up))
    return gate, up, router


def by_collectives(master_gate, second_gate, master_up, second_up, part):
    def moved(master, second):
        narrow = (master + second.astype(jnp.float32)).astype(jnp.bfloat16)
        sent = lax.all_to_all(narrow, "shard", split_axis=2, concat_axis=1, tiled=True)
        return jnp.transpose(sent, (0, 2, 1))

    bands = lax.all_gather(part.T, "shard", axis=0, tiled=True)
    router = lax.all_gather(bands, "expert", axis=1, tiled=True)
    return moved(master_gate, second_gate), moved(master_up, second_up), router


def per_device(n, groups, master_gate, second_gate, master_up, second_up, router_weight, router_gain):
    experts, rows, width = master_gate.shape
    columns = router_weight.shape[1]
    fits = n >= 4 and n % 4 == 0 and groups > 1 and rows % 128 == 0 and width % (16 * n) == 0
    fits = fits and columns % 16 == 0 and min(LATE) >= 2 and experts - max(LATE) > SLOTS
    fits = fits and experts * rows * width * 4 <= 24 * 2**20 and SLOTS * rows * width * 12 <= 7 * 2**20
    fits = fits and n * rows * groups * columns * 2 <= 2**20
    if fits:
        return by_kernel(n, groups, master_gate, second_gate, master_up, second_up, router_weight, router_gain)
    part = (router_weight * router_gain[:, None]).astype(jnp.bfloat16).T
    return by_collectives(master_gate, second_gate, master_up, second_up, part)


def solution(mesh):
    placed = (
        P("expert", "shard", None),
        P("expert", "shard", None),
        P("expert", "shard", None),
        P("expert", "shard", None),
        P("shard", "expert"),
        P("shard"),
    )
    return jax.shard_map(
        functools.partial(per_device, mesh.shape["shard"], mesh.shape["expert"]),
        mesh=mesh,
        in_specs=placed,
        out_specs=(P("expert", "shard", None), P("expert", "shard", None), P()),
        check_vma=False,
    )
```

```python
import functools

import jax
import jax.numpy as jnp
from jax import lax
from jax.experimental import pallas as pl
from jax.experimental.pallas import tpu as pltpu
from jax.sharding import PartitionSpec as P

MESH = pl.DeviceIdType.MESH
SLOTS = 3
LATE = ((6, 2), (2, 0))
EXCHANGE_VMEM = 38 * 2**20
UNLOAD_VMEM = 4 * 2**20


def span(group, experts, phase):
    later = [jnp.where(lax.rem(group, 2) == 0, even, odd) for even, odd in LATE]
    if phase == 0:
        return 0, experts - sum(later)
    return experts - sum(later[phase - 1:]), later[phase - 1]


def exchange_kernel(n, groups, phase, *refs):
    first = phase == 0
    mg, sg, mu, su, *refs = refs
    if first:
        weight, gain, landed, own_block, router, *refs = refs
        wide, narrow, outbox, *refs = refs
        weight_in, gain_in, bands, turned_router, *refs = refs
        in_sem, send_sem, recv_sem, own_out, own_back, router_sem, rs_send, rs_recv, rl_send, rl_recv, re_send, re_recv = refs
    else:
        _, landed, own_block, *refs = refs
        wide, narrow, outbox, in_sem, send_sem, recv_sem, own_out, own_back = refs
    experts, rows, _ = mg.shape
    slots = wide.shape[0]
    block = outbox.shape[3]
    me = lax.axis_index("shard")
    group = lax.axis_index("expert")
    base, count = span(group, experts, phase)

    def body():
        barrier = pltpu.get_barrier_semaphore()
        for j in range(1, n):
            pl.semaphore_signal(barrier, inc=1, device_id=(group, lax.rem(me + j, n)), device_id_type=MESH)
        if first:
            for j in range(1, groups):
                pl.semaphore_signal(barrier, inc=1, device_id=(lax.rem(group + j, groups), me), device_id_type=MESH)

        def load(e):
            slot = lax.rem(e, slots)
            return (
                pltpu.make_async_copy(mg.at[base + e], wide.at[slot, 0], in_sem.at[slot, 0]),
                pltpu.make_async_copy(sg.at[base + e], narrow.at[slot, 0], in_sem.at[slot, 1]),
                pltpu.make_async_copy(mu.at[base + e], wide.at[slot, 1], in_sem.at[slot, 2]),
                pltpu.make_async_copy(su.at[base + e], narrow.at[slot, 1], in_sem.at[slot, 3]),
            )

        for e in range(slots):
            for copy in load(e):
                copy.start()
        cut = pl.ds(pl.multiple_of(me * rows, rows), rows)
        if first:
            router_in = (
                pltpu.make_async_copy(weight, weight_in, router_sem.at[0]),
                pltpu.make_async_copy(gain, gain_in, router_sem.at[1]),
            )
            for copy in router_in:
                copy.start()
            columns = weight.shape[0]
            band = bands.at[pl.ds(pl.multiple_of(group * columns, columns), columns)]
            spot = band.at[:, cut]

        half = n // 2
        lower = me < half
        near = [lax.rem(me + j, half) + jnp.where(lower, 0, half) for j in range(1, half)]
        far = [j + jnp.where(lower, half, 0) for j in range(half)]

        def remote(src, dst, e, peer):
            return pltpu.make_async_remote_copy(
                src_ref=src, dst_ref=dst, send_sem=send_sem.at[e], recv_sem=recv_sem.at[e],
                device_id=(group, peer), device_id_type=MESH,
            )

        def send(e):
            for peer in far + near:
                remote(outbox.at[peer, e], landed.at[e, :, :, cut], e, peer).start()

        def send_half(e, which):
            for peer in far + near:
                remote(outbox.at[peer, e, which], landed.at[e, which, :, cut], e, peer).start()

        def turn(e, which):
            slot = lax.rem(e, slots)
            merged = wide[slot, which] + narrow[slot, which].astype(jnp.float32)
            turned = merged.astype(jnp.bfloat16).T
            for d in range(n):
                outbox[d, e, which] = turned[d * block:(d + 1) * block]

        def step(e, _):
            for copy in load(e):
                copy.wait()
            for which in range(2):
                turn(e, which)

            @pl.when(e + slots < count)
            def _():
                for copy in load(e + slots):
                    copy.start()

            @pl.when(e > 1)
            def _():
                send(e - 1)

            return 0

        opening = load(0)
        for which in range(2):
            for copy in opening[2 * which:2 * which + 2]:
                copy.wait()
            turn(0, which)

        @pl.when(slots < count)
        def _():
            for copy in load(slots):
                copy.start()

        pl.semaphore_wait(barrier, n - 1 + (groups - 1 if first else 0))
        send_half(0, 0)
        if first:
            for copy in router_in:
                copy.wait()
            spot[...] = (weight_in[...] * gain_in[...]).astype(jnp.bfloat16)
        step(1, 0)
        send_half(0, 1)
        if first:
            partner = lax.rem(me + half, n)
            router_rows = []
            for j, peer in enumerate([partner] + near):
                router_rows.append(
                    pltpu.make_async_remote_copy(
                        src_ref=spot, dst_ref=spot, send_sem=rs_send.at[j], recv_sem=rs_recv.at[j],
                        device_id=(group, peer), device_id_type=MESH,
                    )
                )
                router_rows[-1].start()
            lax.fori_loop(2, SLOTS + 1, step, 0)
            router_rows[0].wait()
            passed = band.at[:, pl.ds(pl.multiple_of(partner * rows, rows), rows)]
            for j, peer in enumerate(near):
                router_rows.append(
                    pltpu.make_async_remote_copy(
                        src_ref=passed, dst_ref=passed, send_sem=rl_send.at[j], recv_sem=rl_recv.at[j],
                        device_id=(group, peer), device_id_type=MESH,
                    )
                )
                router_rows[-1].start()
        lax.fori_loop(SLOTS + 1 if first else 2, count, step, 0)
        send(count - 1)

        def leave(e):
            return pltpu.make_async_copy(outbox.at[me, e], own_block.at[e], own_out.at[e])

        def back(e):
            return pltpu.make_async_copy(own_block.at[e], landed.at[e, :, :, cut], own_back.at[e])

        def own_leave(e, _):
            leave(e).start()
            return 0

        def own_return(e, _):
            leave(e).wait()
            back(e).start()
            return 0

        lax.fori_loop(0, count, own_leave, 0)
        lax.fori_loop(0, count, own_return, 0)

        if first:
            for copy in router_rows[1:]:
                copy.wait()
            router_bands = []
            for j in range(1, groups):
                router_bands.append(
                    pltpu.make_async_remote_copy(
                        src_ref=band, dst_ref=band, send_sem=re_send.at[j], recv_sem=re_recv.at[j],
                        device_id=(lax.rem(group + j, groups), me), device_id_type=MESH,
                    )
                )
                router_bands[-1].start()
            for copy in router_bands:
                copy.wait()
            for d in range(n):
                turned_router[d * rows:(d + 1) * rows] = bands[:, d * rows:(d + 1) * rows].T
            out_router = pltpu.make_async_copy(turned_router, router, router_sem.at[0])
            out_router.start()
            out_router.wait()

        def finish(e, _):
            back(e).wait()
            gone = outbox.at[pl.ds(0, n - 1), e]
            pltpu.make_async_copy(gone, gone, send_sem.at[e]).wait()
            come = landed.at[e, :, :, pl.ds(0, (n - 1) * rows)]
            pltpu.make_async_copy(come, come, recv_sem.at[e]).wait()
            return 0

        lax.fori_loop(0, count, finish, 0)

    if first or min(LATE[phase - 1]) > 0:
        body()
    else:
        pl.when(count > 0)(body)


def unload_kernel(phase, *refs):
    first = phase == 0
    last = phase == len(LATE)
    if first:
        landed, router_in, gate, up, token, router, buffer, sem, router_sem = refs
    elif last:
        landed, _, _, gate, up, sem = refs
    else:
        landed, _, _, gate, up, token, sem = refs
    base, count = span(lax.axis_index("expert"), gate.shape[0], phase)

    def copies(e):
        return (
            pltpu.make_async_copy(landed.at[e, 0], gate.at[base + e], sem.at[0, e]),
            pltpu.make_async_copy(landed.at[e, 1], up.at[base + e], sem.at[1, e]),
        )

    def start(e, _):
        for copy in copies(e):
            copy.start()
        return 0

    def wait(e, _):
        for copy in copies(e):
            copy.wait()
        return 0

    if first:
        fetch = pltpu.make_async_copy(router_in, buffer, router_sem.at[0])
        fetch.start()
    lax.fori_loop(0, count, start, 0)
    if not last:
        token[...] = jnp.zeros_like(token)
    if first:
        fetch.wait()
        store = pltpu.make_async_copy(buffer, router, router_sem.at[1])
        store.start()
        store.wait()
    lax.fori_loop(0, count, wait, 0)


def by_kernel(n, groups, master_gate, second_gate, master_up, second_up, router_weight, router_gain):
    experts, rows, width = master_gate.shape
    block = width // n
    columns = router_weight.shape[1]
    anywhere = pl.BlockSpec(memory_space=pl.ANY)
    dma = pltpu.SemaphoreType.DMA
    bf16 = jnp.bfloat16
    whole = jax.ShapeDtypeStruct((experts, block, n * rows), bf16)
    router_shape = (n * rows, groups * columns)
    token_shape = jax.ShapeDtypeStruct((8, 128), jnp.float32)
    stay = functools.partial(pltpu.with_memory_space_constraint, memory_space=pltpu.HBM)
    masters = tuple(stay(x) for x in (master_gate, second_gate, master_up, second_up))

    def exchange(phase, most, more, extra_out, extra_scratch, extra_sems):
        slots = min(SLOTS, *(x for x in LATE[phase - 1] if x)) if phase else SLOTS
        return pl.pallas_call(
            functools.partial(exchange_kernel, n, groups, phase),
            out_shape=(
                pltpu.VMEM((most, 2, block, n * rows), bf16),
                pltpu.HBM((most, 2, block, rows), bf16),
                *extra_out,
            ),
            in_specs=[anywhere] * (4 + len(more)),
            out_specs=(anywhere,) * (2 + len(extra_out)),
            scratch_shapes=[
                pltpu.VMEM((slots, 2, rows, width), jnp.float32),
                pltpu.VMEM((slots, 2, rows, width), bf16),
                pltpu.VMEM((n, most, 2, block, rows), bf16),
                *extra_scratch,
                dma((slots, 4)), dma((most,)), dma((most,)), dma((most,)), dma((most,)),
                *extra_sems,
            ],
            compiler_params=pltpu.CompilerParams(
                collective_id=phase, has_side_effects=True, vmem_limit_bytes=EXCHANGE_VMEM
            ),
        )(*masters, *more)

    most = experts - min(sum(x) for x in zip(*LATE))
    landed, _, router = exchange(
        0, most, (stay(router_weight.T), stay(router_gain[None])),
        (pltpu.HBM(router_shape, bf16),),
        (
            pltpu.VMEM((columns, rows), jnp.float32),
            pltpu.VMEM((1, rows), jnp.float32),
            pltpu.VMEM((groups * columns, n * rows), bf16),
            pltpu.VMEM(router_shape, bf16),
        ),
        (dma((2,)), *[dma((n // 2,))] * 4, dma((groups,)), dma((groups,))),
    )
    in_vmem = pl.BlockSpec(memory_space=pltpu.VMEM)
    unload_params = pltpu.CompilerParams(vmem_limit_bytes=UNLOAD_VMEM)
    gate, up, token, router = pl.pallas_call(
        functools.partial(unload_kernel, 0),
        out_shape=(whole, whole, token_shape, jax.ShapeDtypeStruct(router_shape, bf16)),
        in_specs=[anywhere] * 2,
        out_specs=(anywhere, anywhere, in_vmem, anywhere),
        scratch_shapes=[pltpu.VMEM(router_shape, bf16), dma((2, most)), dma((2,))],
        compiler_params=unload_params,
    )(pltpu.with_memory_space_constraint(landed, pltpu.VMEM), stay(router))
    for phase, late in enumerate(LATE, 1):
        last = phase == len(LATE)
        landed, _ = exchange(phase, max(late), (token,), (), (), ())
        out = pl.pallas_call(
            functools.partial(unload_kernel, phase),
            out_shape=(whole, whole) if last else (whole, whole, token_shape),
            in_specs=[anywhere] * 3,
            out_specs=(anywhere, anywhere) if last else (anywhere, anywhere, in_vmem),
            scratch_shapes=[dma((2, max(late)))],
            input_output_aliases={1: 0, 2: 1},
            compiler_params=unload_params,
        )(pltpu.with_memory_space_constraint(landed, pltpu.VMEM), stay(gate), stay(up))
        gate, up, token = out if not last else (*out, None)
    return gate, up, router


def by_collectives(master_gate, second_gate, master_up, second_up, part):
    def moved(master, second):
        narrow = (master + second.astype(jnp.float32)).astype(jnp.bfloat16)
        sent = lax.all_to_all(narrow, "shard", split_axis=2, concat_axis=1, tiled=True)
        return jnp.transpose(sent, (0, 2, 1))

    bands = lax.all_gather(part.T, "shard", axis=0, tiled=True)
    router = lax.all_gather(bands, "expert", axis=1, tiled=True)
    return moved(master_gate, second_gate), moved(master_up, second_up), router


def per_device(n, groups, master_gate, second_gate, master_up, second_up, router_weight, router_gain):
    experts, rows, width = master_gate.shape
    columns = router_weight.shape[1]
    fits = n >= 4 and n % 4 == 0 and groups > 1 and rows % 128 == 0 and width % (16 * n) == 0
    fits = fits and columns % 16 == 0 and experts - max(sum(x) for x in zip(*LATE)) > SLOTS
    fits = fits and experts * rows * width * 4 <= 24 * 2**20 and SLOTS * rows * width * 12 <= 7 * 2**20
    fits = fits and n * rows * groups * columns * 2 <= 2**20
    if fits:
        return by_kernel(n, groups, master_gate, second_gate, master_up, second_up, router_weight, router_gain)
    part = (router_weight * router_gain[:, None]).astype(jnp.bfloat16).T
    return by_collectives(master_gate, second_gate, master_up, second_up, part)


def solution(mesh):
    placed = (
        P("expert", "shard", None),
        P("expert", "shard", None),
        P("expert", "shard", None),
        P("expert", "shard", None),
        P("shard", "expert"),
        P("shard"),
    )
    return jax.shard_map(
        functools.partial(per_device, mesh.shape["shard"], mesh.shape["expert"]),
        mesh=mesh,
        in_specs=placed,
        out_specs=(P("expert", "shard", None), P("expert", "shard", None), P()),
        check_vma=False,
    )
```

```python
import functools

import jax
import jax.numpy as jnp
from jax import lax
from jax.experimental import pallas as pl
from jax.experimental.pallas import tpu as pltpu
from jax.sharding import PartitionSpec as P

MESH = pl.DeviceIdType.MESH
SLOTS = 3
LATE = ((6, 3), (2, 0))
EXCHANGE_VMEM = 38 * 2**20
UNLOAD_VMEM = 4 * 2**20


def span(group, experts, phase):
    later = [jnp.where(lax.rem(group, 2) == 0, even, odd) for even, odd in LATE]
    if phase == 0:
        return 0, experts - sum(later)
    return experts - sum(later[phase - 1:]), later[phase - 1]


def exchange_kernel(n, groups, phase, *refs):
    first = phase == 0
    mg, sg, mu, su, *refs = refs
    if first:
        weight, gain, landed, own_block, router, *refs = refs
        wide, narrow, outbox, *refs = refs
        weight_in, gain_in, bands, turned_router, *refs = refs
        in_sem, send_sem, recv_sem, own_out, own_back, router_sem, rs_send, rs_recv, rl_send, rl_recv, re_send, re_recv = refs
    else:
        _, landed, own_block, *refs = refs
        wide, narrow, outbox, in_sem, send_sem, recv_sem, own_out, own_back = refs
    experts, rows, _ = mg.shape
    slots = wide.shape[0]
    block = outbox.shape[3]
    me = lax.axis_index("shard")
    group = lax.axis_index("expert")
    base, count = span(group, experts, phase)

    def body():
        barrier = pltpu.get_barrier_semaphore()
        for j in range(1, n):
            pl.semaphore_signal(barrier, inc=1, device_id=(group, lax.rem(me + j, n)), device_id_type=MESH)
        if first:
            for j in range(1, groups):
                pl.semaphore_signal(barrier, inc=1, device_id=(lax.rem(group + j, groups), me), device_id_type=MESH)

        def load(e):
            slot = lax.rem(e, slots)
            return (
                pltpu.make_async_copy(mg.at[base + e], wide.at[slot, 0], in_sem.at[slot, 0]),
                pltpu.make_async_copy(sg.at[base + e], narrow.at[slot, 0], in_sem.at[slot, 1]),
                pltpu.make_async_copy(mu.at[base + e], wide.at[slot, 1], in_sem.at[slot, 2]),
                pltpu.make_async_copy(su.at[base + e], narrow.at[slot, 1], in_sem.at[slot, 3]),
            )

        for e in range(slots):
            for copy in load(e):
                copy.start()
        cut = pl.ds(pl.multiple_of(me * rows, rows), rows)
        if first:
            router_in = (
                pltpu.make_async_copy(weight, weight_in, router_sem.at[0]),
                pltpu.make_async_copy(gain, gain_in, router_sem.at[1]),
            )
            for copy in router_in:
                copy.start()
            columns = weight.shape[0]
            band = bands.at[pl.ds(pl.multiple_of(group * columns, columns), columns)]
            spot = band.at[:, cut]

        half = n // 2
        lower = me < half
        near = [lax.rem(me + j, half) + jnp.where(lower, 0, half) for j in range(1, half)]
        far = [j + jnp.where(lower, half, 0) for j in range(half)]

        def remote(src, dst, e, peer):
            return pltpu.make_async_remote_copy(
                src_ref=src, dst_ref=dst, send_sem=send_sem.at[e], recv_sem=recv_sem.at[e],
                device_id=(group, peer), device_id_type=MESH,
            )

        def send(e):
            for peer in far + near:
                remote(outbox.at[peer, e], landed.at[e, :, :, cut], e, peer).start()

        def send_half(e, which):
            for peer in far + near:
                remote(outbox.at[peer, e, which], landed.at[e, which, :, cut], e, peer).start()

        def turn(e, which):
            slot = lax.rem(e, slots)
            merged = wide[slot, which] + narrow[slot, which].astype(jnp.float32)
            turned = merged.astype(jnp.bfloat16).T
            for d in range(n):
                outbox[d, e, which] = turned[d * block:(d + 1) * block]

        def step(e, _):
            for copy in load(e):
                copy.wait()
            for which in range(2):
                turn(e, which)

            @pl.when(e + slots < count)
            def _():
                for copy in load(e + slots):
                    copy.start()

            @pl.when(e > 1)
            def _():
                send(e - 1)

            return 0

        opening = load(0)
        for which in range(2):
            for copy in opening[2 * which:2 * which + 2]:
                copy.wait()
            turn(0, which)

        @pl.when(slots < count)
        def _():
            for copy in load(slots):
                copy.start()

        pl.semaphore_wait(barrier, n - 1 + (groups - 1 if first else 0))
        send_half(0, 0)
        if first:
            for copy in router_in:
                copy.wait()
            spot[...] = (weight_in[...] * gain_in[...]).astype(jnp.bfloat16)
        step(1, 0)
        send_half(0, 1)
        if first:
            partner = lax.rem(me + half, n)
            router_rows = []
            for j, peer in enumerate([partner] + near):
                router_rows.append(
                    pltpu.make_async_remote_copy(
                        src_ref=spot, dst_ref=spot, send_sem=rs_send.at[j], recv_sem=rs_recv.at[j],
                        device_id=(group, peer), device_id_type=MESH,
                    )
                )
                router_rows[-1].start()
            lax.fori_loop(2, SLOTS + 1, step, 0)
            router_rows[0].wait()
            passed = band.at[:, pl.ds(pl.multiple_of(partner * rows, rows), rows)]
            for j, peer in enumerate(near):
                router_rows.append(
                    pltpu.make_async_remote_copy(
                        src_ref=passed, dst_ref=passed, send_sem=rl_send.at[j], recv_sem=rl_recv.at[j],
                        device_id=(group, peer), device_id_type=MESH,
                    )
                )
                router_rows[-1].start()
        lax.fori_loop(SLOTS + 1 if first else 2, count, step, 0)
        send(count - 1)

        def leave(e):
            return pltpu.make_async_copy(outbox.at[me, e], own_block.at[e], own_out.at[e])

        def back(e):
            return pltpu.make_async_copy(own_block.at[e], landed.at[e, :, :, cut], own_back.at[e])

        def own_leave(e, _):
            leave(e).start()
            return 0

        def own_return(e, _):
            leave(e).wait()
            back(e).start()
            return 0

        lax.fori_loop(0, count, own_leave, 0)
        lax.fori_loop(0, count, own_return, 0)

        if first:
            for copy in router_rows[1:]:
                copy.wait()
            router_bands = []
            for j in range(1, groups):
                router_bands.append(
                    pltpu.make_async_remote_copy(
                        src_ref=band, dst_ref=band, send_sem=re_send.at[j], recv_sem=re_recv.at[j],
                        device_id=(lax.rem(group + j, groups), me), device_id_type=MESH,
                    )
                )
                router_bands[-1].start()
            for copy in router_bands:
                copy.wait()
            for d in range(n):
                turned_router[d * rows:(d + 1) * rows] = bands[:, d * rows:(d + 1) * rows].T
            out_router = pltpu.make_async_copy(turned_router, router, router_sem.at[0])
            out_router.start()
            out_router.wait()

        def finish(e, _):
            back(e).wait()
            gone = outbox.at[pl.ds(0, n - 1), e]
            pltpu.make_async_copy(gone, gone, send_sem.at[e]).wait()
            come = landed.at[e, :, :, pl.ds(0, (n - 1) * rows)]
            pltpu.make_async_copy(come, come, recv_sem.at[e]).wait()
            return 0

        lax.fori_loop(0, count, finish, 0)

    if first or min(LATE[phase - 1]) > 0:
        body()
    else:
        pl.when(count > 0)(body)


def unload_kernel(phase, *refs):
    first = phase == 0
    last = phase == len(LATE)
    if first:
        landed, router_in, gate, up, token, router, buffer, sem, router_sem = refs
    elif last:
        landed, _, _, gate, up, sem = refs
    else:
        landed, _, _, gate, up, token, sem = refs
    base, count = span(lax.axis_index("expert"), gate.shape[0], phase)

    def copies(e):
        return (
            pltpu.make_async_copy(landed.at[e, 0], gate.at[base + e], sem.at[0, e]),
            pltpu.make_async_copy(landed.at[e, 1], up.at[base + e], sem.at[1, e]),
        )

    def start(e, _):
        for copy in copies(e):
            copy.start()
        return 0

    def wait(e, _):
        for copy in copies(e):
            copy.wait()
        return 0

    if first:
        fetch = pltpu.make_async_copy(router_in, buffer, router_sem.at[0])
        fetch.start()
    lax.fori_loop(0, count, start, 0)
    if not last:
        token[...] = jnp.zeros_like(token)
    if first:
        fetch.wait()
        store = pltpu.make_async_copy(buffer, router, router_sem.at[1])
        store.start()
        store.wait()
    lax.fori_loop(0, count, wait, 0)


def by_kernel(n, groups, master_gate, second_gate, master_up, second_up, router_weight, router_gain):
    experts, rows, width = master_gate.shape
    block = width // n
    columns = router_weight.shape[1]
    anywhere = pl.BlockSpec(memory_space=pl.ANY)
    dma = pltpu.SemaphoreType.DMA
    bf16 = jnp.bfloat16
    whole = jax.ShapeDtypeStruct((experts, block, n * rows), bf16)
    router_shape = (n * rows, groups * columns)
    token_shape = jax.ShapeDtypeStruct((8, 128), jnp.float32)
    stay = functools.partial(pltpu.with_memory_space_constraint, memory_space=pltpu.HBM)
    masters = tuple(stay(x) for x in (master_gate, second_gate, master_up, second_up))

    def exchange(phase, most, more, extra_out, extra_scratch, extra_sems):
        slots = min(SLOTS, *(x for x in LATE[phase - 1] if x)) if phase else SLOTS
        return pl.pallas_call(
            functools.partial(exchange_kernel, n, groups, phase),
            out_shape=(
                pltpu.VMEM((most, 2, block, n * rows), bf16),
                pltpu.HBM((most, 2, block, rows), bf16),
                *extra_out,
            ),
            in_specs=[anywhere] * (4 + len(more)),
            out_specs=(anywhere,) * (2 + len(extra_out)),
            scratch_shapes=[
                pltpu.VMEM((slots, 2, rows, width), jnp.float32),
                pltpu.VMEM((slots, 2, rows, width), bf16),
                pltpu.VMEM((n, most, 2, block, rows), bf16),
                *extra_scratch,
                dma((slots, 4)), dma((most,)), dma((most,)), dma((most,)), dma((most,)),
                *extra_sems,
            ],
            compiler_params=pltpu.CompilerParams(
                collective_id=phase, has_side_effects=True, vmem_limit_bytes=EXCHANGE_VMEM
            ),
        )(*masters, *more)

    most = experts - min(sum(x) for x in zip(*LATE))
    landed, _, router = exchange(
        0, most, (stay(router_weight.T), stay(router_gain[None])),
        (pltpu.HBM(router_shape, bf16),),
        (
            pltpu.VMEM((columns, rows), jnp.float32),
            pltpu.VMEM((1, rows), jnp.float32),
            pltpu.VMEM((groups * columns, n * rows), bf16),
            pltpu.VMEM(router_shape, bf16),
        ),
        (dma((2,)), *[dma((n // 2,))] * 4, dma((groups,)), dma((groups,))),
    )
    in_vmem = pl.BlockSpec(memory_space=pltpu.VMEM)
    unload_params = pltpu.CompilerParams(vmem_limit_bytes=UNLOAD_VMEM)
    gate, up, token, router = pl.pallas_call(
        functools.partial(unload_kernel, 0),
        out_shape=(whole, whole, token_shape, jax.ShapeDtypeStruct(router_shape, bf16)),
        in_specs=[anywhere] * 2,
        out_specs=(anywhere, anywhere, in_vmem, anywhere),
        scratch_shapes=[pltpu.VMEM(router_shape, bf16), dma((2, most)), dma((2,))],
        compiler_params=unload_params,
    )(pltpu.with_memory_space_constraint(landed, pltpu.VMEM), stay(router))
    for phase, late in enumerate(LATE, 1):
        last = phase == len(LATE)
        landed, _ = exchange(phase, max(late), (token,), (), (), ())
        out = pl.pallas_call(
            functools.partial(unload_kernel, phase),
            out_shape=(whole, whole) if last else (whole, whole, token_shape),
            in_specs=[anywhere] * 3,
            out_specs=(anywhere, anywhere) if last else (anywhere, anywhere, in_vmem),
            scratch_shapes=[dma((2, max(late)))],
            input_output_aliases={1: 0, 2: 1},
            compiler_params=unload_params,
        )(pltpu.with_memory_space_constraint(landed, pltpu.VMEM), stay(gate), stay(up))
        gate, up, token = out if not last else (*out, None)
    return gate, up, router


def by_collectives(master_gate, second_gate, master_up, second_up, part):
    def moved(master, second):
        narrow = (master + second.astype(jnp.float32)).astype(jnp.bfloat16)
        sent = lax.all_to_all(narrow, "shard", split_axis=2, concat_axis=1, tiled=True)
        return jnp.transpose(sent, (0, 2, 1))

    bands = lax.all_gather(part.T, "shard", axis=0, tiled=True)
    router = lax.all_gather(bands, "expert", axis=1, tiled=True)
    return moved(master_gate, second_gate), moved(master_up, second_up), router


def per_device(n, groups, master_gate, second_gate, master_up, second_up, router_weight, router_gain):
    experts, rows, width = master_gate.shape
    columns = router_weight.shape[1]
    fits = n >= 4 and n % 4 == 0 and groups > 1 and rows % 128 == 0 and width % (16 * n) == 0
    fits = fits and columns % 16 == 0 and experts - max(sum(x) for x in zip(*LATE)) > SLOTS
    fits = fits and experts * rows * width * 4 <= 24 * 2**20 and SLOTS * rows * width * 12 <= 7 * 2**20
    fits = fits and n * rows * groups * columns * 2 <= 2**20
    if fits:
        return by_kernel(n, groups, master_gate, second_gate, master_up, second_up, router_weight, router_gain)
    part = (router_weight * router_gain[:, None]).astype(jnp.bfloat16).T
    return by_collectives(master_gate, second_gate, master_up, second_up, part)


def solution(mesh):
    placed = (
        P("expert", "shard", None),
        P("expert", "shard", None),
        P("expert", "shard", None),
        P("expert", "shard", None),
        P("shard", "expert"),
        P("shard"),
    )
    return jax.shard_map(
        functools.partial(per_device, mesh.shape["shard"], mesh.shape["expert"]),
        mesh=mesh,
        in_specs=placed,
        out_specs=(P("expert", "shard", None), P("expert", "shard", None), P()),
        check_vma=False,
    )
```

```python
import functools

import jax
import jax.numpy as jnp
from jax import lax
from jax.experimental import pallas as pl
from jax.experimental.pallas import tpu as pltpu
from jax.sharding import PartitionSpec as P

MESH = pl.DeviceIdType.MESH
SLOTS = 3
LATE = ((6, 2), (2, 0))
EXCHANGE_VMEM = 38 * 2**20
UNLOAD_VMEM = 4 * 2**20


def span(group, experts, phase):
    later = [jnp.where(lax.rem(group, 2) == 0, even, odd) for even, odd in LATE]
    if phase == 0:
        return 0, experts - sum(later)
    return experts - sum(later[phase - 1:]), later[phase - 1]


def exchange_kernel(n, groups, phase, *refs):
    first = phase == 0
    mg, sg, mu, su, *refs = refs
    if first:
        weight, gain, landed, own_block, router, *refs = refs
        wide, narrow, outbox, *refs = refs
        weight_in, gain_in, bands, turned_router, *refs = refs
        in_sem, send_sem, recv_sem, own_out, own_back, router_sem, rs_send, rs_recv, rl_send, rl_recv, re_send, re_recv = refs
    else:
        _, landed, own_block, *refs = refs
        wide, narrow, outbox, in_sem, send_sem, recv_sem, own_out, own_back = refs
    experts, rows, _ = mg.shape
    slots = wide.shape[0]
    block = outbox.shape[3]
    me = lax.axis_index("shard")
    group = lax.axis_index("expert")
    base, count = span(group, experts, phase)

    def body():
        barrier = pltpu.get_barrier_semaphore()
        for j in range(1, n):
            pl.semaphore_signal(barrier, inc=1, device_id=(group, lax.rem(me + j, n)), device_id_type=MESH)
        if first:
            for j in range(1, groups):
                pl.semaphore_signal(barrier, inc=1, device_id=(lax.rem(group + j, groups), me), device_id_type=MESH)

        def load(e):
            slot = lax.rem(e, slots)
            return (
                pltpu.make_async_copy(mg.at[base + e], wide.at[slot, 0], in_sem.at[slot, 0]),
                pltpu.make_async_copy(sg.at[base + e], narrow.at[slot, 0], in_sem.at[slot, 1]),
                pltpu.make_async_copy(mu.at[base + e], wide.at[slot, 1], in_sem.at[slot, 2]),
                pltpu.make_async_copy(su.at[base + e], narrow.at[slot, 1], in_sem.at[slot, 3]),
            )

        for e in range(slots):
            for copy in load(e):
                copy.start()
        cut = pl.ds(pl.multiple_of(me * rows, rows), rows)
        if first:
            router_in = (
                pltpu.make_async_copy(weight, weight_in, router_sem.at[0]),
                pltpu.make_async_copy(gain, gain_in, router_sem.at[1]),
            )
            for copy in router_in:
                copy.start()
            columns = weight.shape[0]
            band = bands.at[pl.ds(pl.multiple_of(group * columns, columns), columns)]
            spot = band.at[:, cut]

        half = n // 2
        lower = me < half
        near = [lax.rem(me + j, half) + jnp.where(lower, 0, half) for j in range(1, half)]
        far = [jnp.where(lower, j + half if j % 2 == 0 else n - j, j) for j in range(half)]

        def remote(src, dst, e, peer):
            return pltpu.make_async_remote_copy(
                src_ref=src, dst_ref=dst, send_sem=send_sem.at[e], recv_sem=recv_sem.at[e],
                device_id=(group, peer), device_id_type=MESH,
            )

        def send(e):
            for peer in far + near:
                remote(outbox.at[peer, e], landed.at[e, :, :, cut], e, peer).start()

        def send_half(e, which):
            for peer in far + near:
                remote(outbox.at[peer, e, which], landed.at[e, which, :, cut], e, peer).start()

        def turn(e, which):
            slot = lax.rem(e, slots)
            merged = wide[slot, which] + narrow[slot, which].astype(jnp.float32)
            turned = merged.astype(jnp.bfloat16).T
            for d in range(n):
                outbox[d, e, which] = turned[d * block:(d + 1) * block]

        def step(e, _):
            for copy in load(e):
                copy.wait()
            for which in range(2):
                turn(e, which)

            @pl.when(e + slots < count)
            def _():
                for copy in load(e + slots):
                    copy.start()

            @pl.when(e > 1)
            def _():
                send(e - 1)

            return 0

        opening = load(0)
        for which in range(2):
            for copy in opening[2 * which:2 * which + 2]:
                copy.wait()
            turn(0, which)

        @pl.when(slots < count)
        def _():
            for copy in load(slots):
                copy.start()

        pl.semaphore_wait(barrier, n - 1 + (groups - 1 if first else 0))
        send_half(0, 0)
        if first:
            for copy in router_in:
                copy.wait()
            spot[...] = (weight_in[...] * gain_in[...]).astype(jnp.bfloat16)
        step(1, 0)
        send_half(0, 1)
        if first:
            partner = lax.rem(me + half, n)
            router_rows = []
            for j, peer in enumerate([partner] + near):
                router_rows.append(
                    pltpu.make_async_remote_copy(
                        src_ref=spot, dst_ref=spot, send_sem=rs_send.at[j], recv_sem=rs_recv.at[j],
                        device_id=(group, peer), device_id_type=MESH,
                    )
                )
                router_rows[-1].start()
            lax.fori_loop(2, SLOTS + 1, step, 0)
            router_rows[0].wait()
            passed = band.at[:, pl.ds(pl.multiple_of(partner * rows, rows), rows)]
            for j, peer in enumerate(near):
                router_rows.append(
                    pltpu.make_async_remote_copy(
                        src_ref=passed, dst_ref=passed, send_sem=rl_send.at[j], recv_sem=rl_recv.at[j],
                        device_id=(group, peer), device_id_type=MESH,
                    )
                )
                router_rows[-1].start()
        lax.fori_loop(SLOTS + 1 if first else 2, count, step, 0)
        send(count - 1)

        def leave(e):
            return pltpu.make_async_copy(outbox.at[me, e], own_block.at[e], own_out.at[e])

        def back(e):
            return pltpu.make_async_copy(own_block.at[e], landed.at[e, :, :, cut], own_back.at[e])

        def own_leave(e, _):
            leave(e).start()
            return 0

        def own_return(e, _):
            leave(e).wait()
            back(e).start()
            return 0

        lax.fori_loop(0, count, own_leave, 0)
        lax.fori_loop(0, count, own_return, 0)

        if first:
            for copy in router_rows[1:]:
                copy.wait()
            router_bands = []
            for j in range(1, groups):
                router_bands.append(
                    pltpu.make_async_remote_copy(
                        src_ref=band, dst_ref=band, send_sem=re_send.at[j], recv_sem=re_recv.at[j],
                        device_id=(lax.rem(group + j, groups), me), device_id_type=MESH,
                    )
                )
                router_bands[-1].start()
            for copy in router_bands:
                copy.wait()
            for d in range(n):
                turned_router[d * rows:(d + 1) * rows] = bands[:, d * rows:(d + 1) * rows].T
            out_router = pltpu.make_async_copy(turned_router, router, router_sem.at[0])
            out_router.start()
            out_router.wait()

        def finish(e, _):
            back(e).wait()
            gone = outbox.at[pl.ds(0, n - 1), e]
            pltpu.make_async_copy(gone, gone, send_sem.at[e]).wait()
            come = landed.at[e, :, :, pl.ds(0, (n - 1) * rows)]
            pltpu.make_async_copy(come, come, recv_sem.at[e]).wait()
            return 0

        lax.fori_loop(0, count, finish, 0)

    if first or min(LATE[phase - 1]) > 0:
        body()
    else:
        pl.when(count > 0)(body)


def unload_kernel(phase, *refs):
    first = phase == 0
    last = phase == len(LATE)
    if first:
        landed, router_in, gate, up, token, router, buffer, sem, router_sem = refs
    elif last:
        landed, _, _, gate, up, sem = refs
    else:
        landed, _, _, gate, up, token, sem = refs
    base, count = span(lax.axis_index("expert"), gate.shape[0], phase)

    def copies(e):
        return (
            pltpu.make_async_copy(landed.at[e, 0], gate.at[base + e], sem.at[0, e]),
            pltpu.make_async_copy(landed.at[e, 1], up.at[base + e], sem.at[1, e]),
        )

    def start(e, _):
        for copy in copies(e):
            copy.start()
        return 0

    def wait(e, _):
        for copy in copies(e):
            copy.wait()
        return 0

    if first:
        fetch = pltpu.make_async_copy(router_in, buffer, router_sem.at[0])
        fetch.start()
    lax.fori_loop(0, count, start, 0)
    if not last:
        token[...] = jnp.zeros_like(token)
    if first:
        fetch.wait()
        store = pltpu.make_async_copy(buffer, router, router_sem.at[1])
        store.start()
        store.wait()
    lax.fori_loop(0, count, wait, 0)


def by_kernel(n, groups, master_gate, second_gate, master_up, second_up, router_weight, router_gain):
    experts, rows, width = master_gate.shape
    block = width // n
    columns = router_weight.shape[1]
    anywhere = pl.BlockSpec(memory_space=pl.ANY)
    dma = pltpu.SemaphoreType.DMA
    bf16 = jnp.bfloat16
    whole = jax.ShapeDtypeStruct((experts, block, n * rows), bf16)
    router_shape = (n * rows, groups * columns)
    token_shape = jax.ShapeDtypeStruct((8, 128), jnp.float32)
    stay = functools.partial(pltpu.with_memory_space_constraint, memory_space=pltpu.HBM)
    masters = tuple(stay(x) for x in (master_gate, second_gate, master_up, second_up))

    def exchange(phase, most, more, extra_out, extra_scratch, extra_sems):
        slots = min(SLOTS, *(x for x in LATE[phase - 1] if x)) if phase else SLOTS
        return pl.pallas_call(
            functools.partial(exchange_kernel, n, groups, phase),
            out_shape=(
                pltpu.VMEM((most, 2, block, n * rows), bf16),
                pltpu.HBM((most, 2, block, rows), bf16),
                *extra_out,
            ),
            in_specs=[anywhere] * (4 + len(more)),
            out_specs=(anywhere,) * (2 + len(extra_out)),
            scratch_shapes=[
                pltpu.VMEM((slots, 2, rows, width), jnp.float32),
                pltpu.VMEM((slots, 2, rows, width), bf16),
                pltpu.VMEM((n, most, 2, block, rows), bf16),
                *extra_scratch,
                dma((slots, 4)), dma((most,)), dma((most,)), dma((most,)), dma((most,)),
                *extra_sems,
            ],
            compiler_params=pltpu.CompilerParams(
                collective_id=phase, has_side_effects=True, vmem_limit_bytes=EXCHANGE_VMEM
            ),
        )(*masters, *more)

    most = experts - min(sum(x) for x in zip(*LATE))
    landed, _, router = exchange(
        0, most, (stay(router_weight.T), stay(router_gain[None])),
        (pltpu.HBM(router_shape, bf16),),
        (
            pltpu.VMEM((columns, rows), jnp.float32),
            pltpu.VMEM((1, rows), jnp.float32),
            pltpu.VMEM((groups * columns, n * rows), bf16),
            pltpu.VMEM(router_shape, bf16),
        ),
        (dma((2,)), *[dma((n // 2,))] * 4, dma((groups,)), dma((groups,))),
    )
    in_vmem = pl.BlockSpec(memory_space=pltpu.VMEM)
    unload_params = pltpu.CompilerParams(vmem_limit_bytes=UNLOAD_VMEM)
    gate, up, token, router = pl.pallas_call(
        functools.partial(unload_kernel, 0),
        out_shape=(whole, whole, token_shape, jax.ShapeDtypeStruct(router_shape, bf16)),
        in_specs=[anywhere] * 2,
        out_specs=(anywhere, anywhere, in_vmem, anywhere),
        scratch_shapes=[pltpu.VMEM(router_shape, bf16), dma((2, most)), dma((2,))],
        compiler_params=unload_params,
    )(pltpu.with_memory_space_constraint(landed, pltpu.VMEM), stay(router))
    for phase, late in enumerate(LATE, 1):
        last = phase == len(LATE)
        landed, _ = exchange(phase, max(late), (token,), (), (), ())
        out = pl.pallas_call(
            functools.partial(unload_kernel, phase),
            out_shape=(whole, whole) if last else (whole, whole, token_shape),
            in_specs=[anywhere] * 3,
            out_specs=(anywhere, anywhere) if last else (anywhere, anywhere, in_vmem),
            scratch_shapes=[dma((2, max(late)))],
            input_output_aliases={1: 0, 2: 1},
            compiler_params=unload_params,
        )(pltpu.with_memory_space_constraint(landed, pltpu.VMEM), stay(gate), stay(up))
        gate, up, token = out if not last else (*out, None)
    return gate, up, router


def by_collectives(master_gate, second_gate, master_up, second_up, part):
    def moved(master, second):
        narrow = (master + second.astype(jnp.float32)).astype(jnp.bfloat16)
        sent = lax.all_to_all(narrow, "shard", split_axis=2, concat_axis=1, tiled=True)
        return jnp.transpose(sent, (0, 2, 1))

    bands = lax.all_gather(part.T, "shard", axis=0, tiled=True)
    router = lax.all_gather(bands, "expert", axis=1, tiled=True)
    return moved(master_gate, second_gate), moved(master_up, second_up), router


def per_device(n, groups, master_gate, second_gate, master_up, second_up, router_weight, router_gain):
    experts, rows, width = master_gate.shape
    columns = router_weight.shape[1]
    fits = n >= 4 and n % 4 == 0 and groups > 1 and rows % 128 == 0 and width % (16 * n) == 0
    fits = fits and columns % 16 == 0 and experts - max(sum(x) for x in zip(*LATE)) > SLOTS
    fits = fits and experts * rows * width * 4 <= 24 * 2**20 and SLOTS * rows * width * 12 <= 7 * 2**20
    fits = fits and n * rows * groups * columns * 2 <= 2**20
    if fits:
        return by_kernel(n, groups, master_gate, second_gate, master_up, second_up, router_weight, router_gain)
    part = (router_weight * router_gain[:, None]).astype(jnp.bfloat16).T
    return by_collectives(master_gate, second_gate, master_up, second_up, part)


def solution(mesh):
    placed = (
        P("expert", "shard", None),
        P("expert", "shard", None),
        P("expert", "shard", None),
        P("expert", "shard", None),
        P("shard", "expert"),
        P("shard"),
    )
    return jax.shard_map(
        functools.partial(per_device, mesh.shape["shard"], mesh.shape["expert"]),
        mesh=mesh,
        in_specs=placed,
        out_specs=(P("expert", "shard", None), P("expert", "shard", None), P()),
        check_vma=False,
    )
```
